32 devices in a mesh: seq: 4 (over y, core), head: 8 (over z, x).
Axes of the slice: x: 2, y: 2, z: 4, core: 2. Of those that a mesh axis runs over, the one named last changes fastest.
Arguments:
- queries: bfloat16 [8, 2048, 256], P('head', 'seq'), may hold values from -6 to 6
- keys: bfloat16 [1, 2048, 256], P(None, 'seq'), may hold values from -6 to 6
- values: bfloat16 [1, 2048, 256], P(None, 'seq'), may hold values from -6 to 6
- d_out: bfloat16 [8, 2048, 256], P('head', 'seq'), may hold values from -12 to 12
- doc_lengths: int32 [1, 8], replicated, may hold values from 1 to 768, 2048 in all within a row
- fold_order: int32 [8], replicated, may hold values from 0 to 7, each once
Outputs:
- grad_queries: bfloat16 [8, 2048, 256], P('head', 'seq')
- grad_keys: float32 [1, 2048, 256], P(None, ('seq', 'head'))
- grad_values: float32 [1, 2048, 256], P(None, ('seq', 'head'))
The draws below stay inside these ranges and needn't reach their ends.
Inputs may be any that keep to these rules, and one draw needn't show every extreme that they name: `doc_lengths`: each row's 8 lengths are at least 1, sum to 2048, and the longest is exactly 768. fold_order names each of 0 to 7 once.
All inputs are finite; a program needn't handle non-finite values.
Results may differ from the reference program's by a relative error of at most 0.029.
Values may be sent and summed in bfloat16 or wider, within the bound.
A program may use at most 64 MiB of HBM per device.

```python
import math
import jax
import jax.numpy as jnp
import numpy as np

HEAD_COUNT = 8
HEAD_DIM = 256
DOC_COUNT = 8
SEQ_LEN = 2048
BLOCK_LEN = 256
BLOCK_COUNT = 8
PACKED_ROWS = 1
ROW_HEADS = 8
DOC_MOST = 768


def draw_queries(key, part):
    full_shape = (ROW_HEADS, SEQ_LEN, HEAD_DIM)
    drawn = jnp.clip(jax.random.normal(jax.random.fold_in(key, 3), full_shape, jnp.float32), -6.0, 6.0)
    return drawn.astype(jnp.bfloat16)


def draw_keys(key, part):
    full_shape = (PACKED_ROWS, SEQ_LEN, HEAD_DIM)
    drawn = jnp.clip(jax.random.normal(jax.random.fold_in(key, 5), full_shape, jnp.float32), -6.0, 6.0)
    return drawn.astype(jnp.bfloat16)


def block_levels(key, dims, pieces, smallest, largest):
    factor_of, own = 1.0, jax.random.fold_in(key, 6)
    for dim, blocks in pieces:
        heights = jnp.exp(jax.random.uniform(jax.random.fold_in(own, dim), (blocks,), jnp.float32, smallest / len(pieces), largest / len(pieces)))
        factor_of = factor_of * jnp.repeat(heights, dims[dim] // blocks).reshape([-1 if axis == dim else 1 for axis in range(len(dims))])
    return factor_of


def length_profile(number_of, total, reach, lean):
    loads = [(1 << 20) // math.isqrt(standing ** lean) + 1 for standing in range(2, number_of + 1)]
    spare, counts = total - reach - (number_of - 1), [1] * (number_of - 1)
    while spare > 0:
        candidates = [i for i in range(number_of - 1) if counts[i] < reach]
        whole, budget = sum([loads[i] for i in candidates]), spare
        for i in candidates:
            more = min(reach - counts[i], max(1, budget * loads[i] // whole), spare)
            counts[i] = counts[i] + more
            spare = spare - more
    return np.array([reach] + counts)


def uneven_parts(key, amount, total, most, slope):
    if amount == 2:
        one = jax.random.randint(key, (), max(1, total - most), min(most, total - 1) + 1)
        return jnp.stack([one, total - one])
    tallies = jnp.asarray(length_profile(amount, total, most, slope), jnp.int32)
    pairs = (amount - 1) // 2
    donor, taker = tallies[1:1 + 2 * pairs:2], tallies[2:2 + 2 * pairs:2]
    room = jnp.minimum(donor - 1, most - taker)
    shifted = jax.random.randint(jax.random.fold_in(key, 1), (pairs,), 0, 1 << 20) % (room + 1)
    tallies = tallies.at[1:1 + 2 * pairs:2].set(donor - shifted).at[2:2 + 2 * pairs:2].set(taker + shifted)
    return tallies[jax.random.permutation(jax.random.fold_in(key, 2), amount)]


def bell_draw(stream_key, dims, spread, most, split=(), kind=jnp.bfloat16):
    array = spread * jax.random.normal(stream_key, dims, jnp.float32)
    if split:
        array = array * block_levels(stream_key, dims, split, -0.22, 0.18)
    return jnp.clip(array, -most, most).astype(kind)


def setup_inputs(seed: int = 0) -> dict:
    key_of = jax.random.split(jax.random.key(seed), 7)
    queries = draw_queries(jax.random.fold_in(key_of[6], 71), 0)
    keys = draw_keys(jax.random.fold_in(key_of[6], 71), 0)
    values = bell_draw(key_of[2], (PACKED_ROWS, SEQ_LEN, HEAD_DIM), 1.0, 6.0, ((1, 4),))
    d_out = bell_draw(key_of[3], (ROW_HEADS, SEQ_LEN, HEAD_DIM), 2.0, 12.0, ((0, 8), (1, 4)))
    doc_lengths = jax.vmap(lambda own: uneven_parts(own, DOC_COUNT, SEQ_LEN, DOC_MOST, 2))(jax.random.split(key_of[4], PACKED_ROWS)).reshape((PACKED_ROWS, DOC_COUNT)).astype(jnp.int32)
    fold_order = jax.random.permutation(key_of[5], BLOCK_COUNT).astype(jnp.int32)
    return {"queries": queries, "keys": keys, "values": values, "d_out": d_out, "doc_lengths": doc_lengths, "fold_order": fold_order}


masked_value = -1e30


def reference(queries, keys, values, d_out, doc_lengths, fold_order):
    scaling = HEAD_DIM ** -0.5
    indices = jnp.arange(SEQ_LEN, dtype=jnp.int32)
    position = fold_order[indices // BLOCK_LEN] * BLOCK_LEN + indices % BLOCK_LEN
    query_grads = []
    key_grads = []
    value_grads = []
    for row_index in range(PACKED_ROWS):
        lengths = doc_lengths[row_index]
        starts = jnp.cumsum(lengths, dtype=jnp.int32) - lengths
        document = jnp.sum((position[:, None] >= starts[None, :]).astype(jnp.int32), axis=1, dtype=jnp.int32)
        allowed = (document[:, None] == document[None, :]) & (position[None, :] <= position[:, None])
        key_row = keys[row_index]
        value_row = values[row_index]
        key_total = jnp.zeros((SEQ_LEN, HEAD_DIM), jnp.float32)
        value_total = jnp.zeros((SEQ_LEN, HEAD_DIM), jnp.float32)
        for head_index in range(HEAD_COUNT):
            pair_index = row_index * HEAD_COUNT + head_index
            query_rows = queries[pair_index]
            grad_out = d_out[pair_index]
            scores = jnp.where(allowed, jnp.dot(query_rows, key_row.T, preferred_element_type=jnp.float32) * scaling, masked_value)
            row_max = jnp.max(scores, axis=1, keepdims=True)
            log_norm = row_max + jnp.log(jnp.sum(jnp.exp(scores - row_max), axis=1, keepdims=True))
            weights = jnp.exp(scores - log_norm)
            weights_low = weights.astype(jnp.bfloat16)
            output = jnp.dot(weights_low, value_row, preferred_element_type=jnp.float32)
            grad_dot = jnp.sum(grad_out.astype(jnp.float32) * output, axis=1, keepdims=True)
            grad_prob = jnp.dot(grad_out, value_row.T, preferred_element_type=jnp.float32)
            grad_score = (weights * (grad_prob - grad_dot)).astype(jnp.bfloat16)
            query_grads.append((jnp.dot(grad_score, key_row, preferred_element_type=jnp.float32) * scaling).astype(jnp.bfloat16))
            key_total = key_total + jnp.dot(grad_score.T, query_rows, preferred_element_type=jnp.float32) * scaling
            value_total = value_total + jnp.dot(weights_low.T, grad_out, preferred_element_type=jnp.float32)
        key_grads.append(key_total)
        value_grads.append(value_total)
    return jnp.stack(query_grads), jnp.stack(key_grads), jnp.stack(value_grads)
```

```python
import functools

import jax
import jax.numpy as jnp
from jax import lax
from jax.experimental import pallas as pl
from jax.experimental.pallas import tpu as pltpu
from jax.sharding import PartitionSpec as P

HEAD_COUNT = 8


masked_value = -1e30


def contract_last(left, right):
    return lax.dot_general(
        left, right, (((1,), (1,)), ((), ())), preferred_element_type=jnp.float32
    )


def contract_first(left, right):
    return lax.dot_general(
        left, right, (((0,), (0,)), ((), ())), preferred_element_type=jnp.float32
    )


def block_grads(query_rows, grad_out, log_norm, grad_dot, key_part, value_part, allowed, scaling):
    scores = contract_last(query_rows, key_part) * scaling
    weights = jnp.exp(jnp.where(allowed, scores - log_norm, masked_value))
    weights_low = weights.astype(jnp.bfloat16)
    grad_prob = contract_last(grad_out, value_part)
    grad_score = (weights * (grad_prob - grad_dot)).astype(jnp.bfloat16)
    part_query = jnp.dot(grad_score, key_part, preferred_element_type=jnp.float32) * scaling
    part_key = contract_first(grad_score, query_rows) * scaling
    part_value = contract_first(weights_low, grad_out)
    return (part_query, part_key, part_value)


def owner_blocks(key_part, value_part, row_count):
    head_total = lax.axis_size("head")
    piece_len = key_part.shape[0] // head_total
    width = key_part.shape[1]
    moved = (
        lax.all_to_all(
            key_part.astype(jnp.bfloat16), "head", split_axis=0, concat_axis=0, tiled=True
        ).astype(key_part.dtype),
        lax.all_to_all(
            value_part.astype(jnp.bfloat16), "head", split_axis=0, concat_axis=0, tiled=True
        ).astype(value_part.dtype),
    )
    return tuple(
        (
            jnp.sum(item.reshape(row_count, head_total // row_count, piece_len, width), axis=1)
            for item in moved
        )
    )


def per_device(queries, keys, values, d_out, doc_lengths, fold_order):
    local_len = queries.shape[1]
    head_width = queries.shape[2]
    half_len = local_len // 2
    scaling = head_width ** (-0.5)
    seq_index = lax.axis_index("seq")
    row_index = lax.axis_index("head") // HEAD_COUNT
    row_count = keys.shape[0]
    span_ids = jnp.arange(fold_order.shape[0], dtype=jnp.int32)
    lengths = lax.dynamic_index_in_dim(doc_lengths, row_index, 0, keepdims=False)
    starts = jnp.cumsum(lengths, dtype=jnp.int32) - lengths

    def locate(indices):
        block_of = indices // half_len
        anchor = jnp.sum(
            jnp.where(block_of[:, None] == span_ids[None, :], fold_order[None, :], 0),
            axis=1,
            dtype=jnp.int32,
        )
        position = anchor * half_len + indices % half_len
        document = jnp.sum(
            (position[:, None] >= starts[None, :]).astype(jnp.int32), axis=1, dtype=jnp.int32
        )
        return (position, document)

    def allowed_pairs(query_place, key_place):
        return (query_place[1][:, None] == key_place[1][None, :]) & (
            key_place[0][None, :] <= query_place[0][:, None]
        )

    local_rows = jnp.arange(local_len, dtype=jnp.int32)
    own_place = locate(seq_index * local_len + local_rows)
    query_rows = queries[0]
    grad_out = d_out[0]
    key_row = lax.dynamic_index_in_dim(keys, row_index, 0, keepdims=False)
    value_row = lax.dynamic_index_in_dim(values, row_index, 0, keepdims=False)
    key_part = lax.all_gather(key_row, "seq", axis=0, tiled=True)
    value_part = lax.all_gather(value_row, "seq", axis=0, tiled=True)
    allowed = allowed_pairs(own_place, locate(jnp.arange(key_part.shape[0], dtype=jnp.int32)))
    run_max = jnp.full((local_len, 1), masked_value, jnp.float32)
    scores = jnp.where(allowed, contract_last(query_rows, key_part) * scaling, masked_value)
    new_max = jnp.maximum(run_max, jnp.max(scores, axis=1, keepdims=True))
    weights = jnp.where(allowed, jnp.exp(scores - new_max), 0.0)
    sum_next = jnp.sum(weights, axis=1, keepdims=True)
    acc_next = jnp.dot(weights.astype(jnp.bfloat16), value_part, preferred_element_type=jnp.float32)
    log_norm = new_max + jnp.log(sum_next)
    output = acc_next / sum_next
    grad_dot = jnp.sum(grad_out.astype(jnp.float32) * output, axis=1, keepdims=True)
    key_part = lax.all_gather(key_row, "seq", axis=0, tiled=True)
    value_part = lax.all_gather(value_row, "seq", axis=0, tiled=True)
    row_total = key_part.shape[0]
    allowed = allowed_pairs(own_place, locate(jnp.arange(row_total, dtype=jnp.int32)))
    part_query, part_key, part_value = block_grads(
        query_rows, grad_out, log_norm, grad_dot, key_part, value_part, allowed, scaling
    )
    full_keys = part_key
    full_values = part_value
    grad_query, full_keys, full_values = (part_query, full_keys, full_values)
    seq_keys, seq_values = (
        lax.psum_scatter(
            full_keys.astype(jnp.bfloat16), "seq", scatter_dimension=0, tiled=True
        ).astype(jnp.float32),
        lax.psum_scatter(
            full_values.astype(jnp.bfloat16), "seq", scatter_dimension=0, tiled=True
        ).astype(jnp.float32),
    )
    grad_keys, grad_values = owner_blocks(seq_keys, seq_values, row_count)
    grad_queries = grad_query.astype(jnp.bfloat16)[None]
    return (grad_queries, grad_keys, grad_values)


MESH = pl.DeviceIdType.MESH


def fused_kernel(
    z_count,
    q_hbm,
    k_hbm,
    v_hbm,
    o_hbm,
    len_hbm,
    fold_hbm,
    gq_ref,
    gk_ref,
    gv_ref,
    q_ref,
    o_ref,
    q_low,
    len_ref,
    fold_ref,
    load,
    kv,
    scores,
    probs,
    top_at,
    p_low,
    ds_low,
    k_sorted,
    stat_out,
    stat_in,
    own,
    first_out,
    first_in,
    next_out,
    next_in,
    z_out,
    z_in,
    gq_out,
    gq_in,
    send,
    recv,
    z_send,
    z_recv,
    ready,
):
    rows, width = k_hbm.shape
    scaling = width ** (-0.5)
    block_total = fold_ref.shape[0]
    doc_total = len_ref.shape[1]
    blocks = block_total // 4
    block_len = rows // blocks
    group = rows // z_count
    piece = group // 2
    part = rows // 4
    bf16 = jnp.bfloat16
    f32 = jnp.float32

    seq = lax.axis_index("seq")
    head = lax.axis_index("head")
    y, c = seq // 2, seq % 2
    z, x = head // 2, head % 2
    partner = {"seq": y * 2 + (1 - c), "head": head}
    y_peer = {"seq": (1 - y) * 2 + c, "head": head}
    x_peer = {"seq": seq, "head": z * 2 + (1 - x)}

    barrier = pltpu.get_barrier_semaphore()
    for peer in (partner, y_peer, x_peer):
        pl.semaphore_signal(barrier, inc=1, device_id=peer, device_id_type=MESH)

    def tell_line(semaphore):
        @pl.when(z > 0)
        def _():
            pl.semaphore_signal(
                semaphore,
                inc=1,
                device_id={"seq": seq, "head": (z - 1) * 2 + x},
                device_id_type=MESH,
            )

        @pl.when(z < z_count - 1)
        def _():
            pl.semaphore_signal(
                semaphore,
                inc=1,
                device_id={"seq": seq, "head": (z + 1) * 2 + x},
                device_id_type=MESH,
            )

    line_peers = (z + z_count - 1) // z_count + (2 * z_count - 2 - z) // z_count
    tell_line(barrier)

    near_half = pl.ds(0, rows)
    far_half = pl.ds(rows, rows)
    loads = [
        pltpu.make_async_copy(src, dst, load.at[i])
        for i, (src, dst) in enumerate(
            (
                (k_hbm, kv.at[0, 0]),
                (v_hbm, kv.at[0, 1]),
                (q_hbm, q_ref.at[near_half]),
                (o_hbm, o_ref.at[near_half]),
                (fold_hbm, fold_ref),
                (len_hbm, len_ref),
            )
        )
    ]
    for copy in loads:
        copy.start()

    issued = []

    def remote(src, dst, peer):
        i = len(issued)
        copy = pltpu.make_async_remote_copy(
            src_ref=src,
            dst_ref=dst,
            send_sem=send.at[i],
            recv_sem=recv.at[i],
            device_id=peer,
            device_id_type=MESH,
        )
        copy.start()
        issued.append(copy)
        return copy

    def is_at(at):
        return 1 // (1 + (z - at) * (z - at))

    tables = [
        sorted(range(z_count), key=lambda to: (-abs(to - at), to)) for at in range(z_count)
    ]
    farthest = [
        sum(tables[at][j] * is_at(at) for at in range(z_count)) for j in range(z_count)
    ]

    pl.semaphore_wait(barrier, 3 + line_peers)

    z_low = z % 2
    z_pair = {"seq": seq, "head": (z + 1 - 2 * z_low) * 2 + x}

    def quarter(flip_x, flip_z):
        at_x = 1 - x if flip_x else x
        at_z = 1 - z_low if flip_z else z_low
        return pl.multiple_of((at_x * 2 + at_z) * part, part)

    y_copies = []
    for i in range(4):
        at = pl.ds(quarter(i // 2, i // 2), part)
        if i < 2:
            loads[i].wait()
        y_copies.append(remote(kv.at[0, i % 2, at], kv.at[1, i % 2, at], y_peer))
    loads[2].wait()
    q_copy = remote(q_ref.at[near_half], q_ref.at[far_half], partner)
    loads[3].wait()
    o_copy = remote(o_ref.at[near_half], o_ref.at[far_half], partner)
    tell_line(ready.at[0])
    for copy in loads[4:]:
        copy.wait()

    lane = lax.broadcasted_iota(jnp.int32, (1, 2 * rows), 1)
    place = jnp.zeros((1, 2 * rows), jnp.int32)
    mate = y * 2 + (1 - c)
    for b in range(2 * blocks):
        index = seq * blocks + b if b < blocks else mate * blocks + b - blocks
        at = fold_ref[index] * block_len + lane - b * block_len
        place = jnp.where(lane // block_len == b, at, place)
    first = jnp.zeros((1, 2 * rows), jnp.int32)
    start = jnp.int32(0)
    for d in range(doc_total):
        first = jnp.where(place >= start, start, first)
        start = start + len_ref[0, d]

    tops, sums, dots = [[], []], [[], []], [[], []]

    def take_keys(slot, off, count, half):
        shard = seq if slot == 0 else (1 - y) * 2 + c
        cols = slice(half * rows, (half + 1) * rows)
        at = pl.ds(off, count)
        base = fold_ref[shard * blocks + off // block_len] * block_len + off % block_len
        depth = lax.broadcasted_iota(jnp.int32, (count, rows), 0)
        item = contract_last(kv[slot, 0, at], q_low[cols])
        seen = (depth >= first[:, cols] - base) & (depth <= place[:, cols] - base)
        item = jnp.where(seen, item, masked_value)
        top = jnp.max(item, axis=0, keepdims=True)
        item = jnp.exp(item - top)
        scores[slot, at, cols] = item
        for b in range(count // part):
            top_at[slot, off // part + b, :, cols] = top
        tops[half].append(top)
        sums[half].append(jnp.sum(item, axis=0, keepdims=True))

    def take_values(slot, off, count, half):
        cols = slice(half * rows, (half + 1) * rows)
        at = pl.ds(off, count)
        item = contract_last(kv[slot, 1, at], o_ref[cols])
        probs[slot, at, cols] = item
        dots[half].append(jnp.sum(scores[slot, at, cols] * item, axis=0, keepdims=True))

    def line_step(step):
        pl.semaphore_wait(ready.at[step], line_peers)
        if step + 1 < z_count - 2:
            tell_line(ready.at[step + 1])

    q_low[0:rows] = (q_ref[0:rows].astype(f32) * scaling).astype(bf16)
    for b in range(blocks):
        take_keys(0, b * block_len, block_len, 0)
        take_values(0, b * block_len, block_len, 0)

    line_step(0)
    q_copy.wait_recv()
    q_low[rows : 2 * rows] = (q_ref[rows : 2 * rows].astype(f32) * scaling).astype(bf16)
    for b in range(blocks):
        take_keys(0, b * block_len, block_len, 1)

    x_copies, z_copies = [], []

    def relay(i):
        y_copies[i].wait_recv()
        block = kv.at[1, i, pl.ds(quarter(0, 0), part)]
        x_copies.append(remote(block, block, x_peer))
        z_copies.append(remote(block, block, z_pair))

    def take_far(take, flip_x, flip_z):
        for half in range(2):
            take(1, quarter(flip_x, flip_z), part, half)

    relay(0)
    o_copy.wait_recv()
    for b in range(blocks):
        take_values(0, b * block_len, block_len, 1)
    take_far(take_keys, 0, 0)
    relay(1)
    take_far(take_values, 0, 0)
    y_copies[2].wait_recv()
    take_far(take_keys, 1, 1)
    z_copies[0].wait_recv()
    take_far(take_keys, 0, 1)
    x_copies[0].wait_recv()
    take_far(take_keys, 1, 0)

    def swapped(i):
        return jnp.concatenate(
            [stat_in[i, :, rows : 2 * rows], stat_in[i, :, 0:rows]], axis=1
        )

    log_sums = []
    for half in range(2):
        top = functools.reduce(jnp.maximum, tops[half])
        total = sum(s * jnp.exp(t - top) for s, t in zip(sums[half], tops[half]))
        log_sums.append(top + jnp.log(total))
        stat_out[0, :, half * rows : (half + 1) * rows] = log_sums[half]
    norm_copy = remote(stat_out.at[0], stat_in.at[0], partner)
    for step in range(1, z_count - 2):
        line_step(step)

    y_copies[3].wait_recv()
    take_far(take_values, 1, 1)
    z_copies[1].wait_recv()
    take_far(take_values, 0, 1)
    x_copies[1].wait_recv()
    take_far(take_values, 1, 0)

    for half in range(2):
        stat_out[1, :, half * rows : (half + 1) * rows] = sum(
            d * jnp.exp(t - log_sums[half]) for d, t in zip(dots[half], tops[half])
        )
    dot_copy = remote(stat_out.at[1], stat_in.at[1], partner)

    def pieces(j):
        mine = pl.ds(pl.multiple_of(farthest[j] * group + x * piece, piece), piece)
        other = pl.ds(pl.multiple_of(farthest[j] * group + (1 - x) * piece, piece), piece)
        return [(0, mine), (0, other), (1, mine), (1, other)]

    def first_hop(u, item, x_first):
        near_mine, near_other, far_mine, far_other = (
            item[i * piece : (i + 1) * piece] for i in range(4)
        )
        kept, sent = (far_mine, near_other) if x_first else (near_other, far_mine)
        own[u, 0:piece] = near_mine
        own[u, piece:group] = kept
        first_out[u, 0:piece] = sent.astype(bf16)
        first_out[u, piece:group] = far_other.astype(bf16)
        peers = (x_peer, y_peer) if x_first else (y_peer, x_peer)
        return (remote(first_out.at[u], first_in.at[u], peers[0]), peers[1])

    def second_hop(u, hop):
        hop[0].wait_recv()
        next_out[u] = (own[u, piece:group] + first_in[u, piece:group].astype(f32)).astype(bf16)
        return remote(next_out.at[u], next_in.at[u], hop[1])

    z_copies_out = []

    def z_copy(n, j, d):
        return pltpu.make_async_remote_copy(
            src_ref=z_out.at[n, j],
            dst_ref=z_in.at[n, d],
            send_sem=z_send.at[n, j],
            recv_sem=z_recv.at[n, d],
            device_id={"seq": seq, "head": ((z + d + 1) % z_count) * 2 + x},
            device_id_type=MESH,
        )

    def third_hop(u, copy):
        n, j = u // z_count, u % z_count
        copy.wait_recv()
        item = own[u, 0:piece] + first_in[u, 0:piece].astype(f32) + next_in[u].astype(f32)
        if j == z_count - 1:
            return item
        z_out[n, j] = item.astype(bf16)
        move = z_copy(n, j, (farthest[j] - z + z_count - 1) % z_count)
        move.start()
        z_copies_out.append(move)
        return None

    for j in range(z_count):
        for i, (slot, at) in enumerate(pieces(j)):
            k_sorted[j * 2 * group + i * piece : j * 2 * group + (i + 1) * piece] = kv[slot, 0, at]

    norm_copy.wait_recv()
    mine, theirs = stat_out[0], swapped(0)
    top = jnp.maximum(mine, theirs)
    log_norm = top + jnp.log(jnp.exp(mine - top) + jnp.exp(theirs - top))
    for slot in range(2):
        for b in range(4):
            top_at[slot, b] = jnp.exp(top_at[slot, b] - log_norm)

    hops = {}

    def value_part(j):
        for i, (slot, at) in enumerate(pieces(j)):
            weights = scores[slot, at] * top_at[slot, farthest[j]]
            scores[slot, at] = weights
            p_low[j, i * piece : (i + 1) * piece] = weights.astype(bf16)
        item = jnp.dot(p_low[j], o_ref[...], preferred_element_type=f32)
        hops[j] = first_hop(j, item, j % 2 == 0)

    for j in range(z_count - 1):
        value_part(j)
    dot_copy.wait_recv()
    grad_dot = stat_out[1] * jnp.exp(mine - log_norm) + swapped(1) * jnp.exp(theirs - log_norm)

    def key_part(j):
        for i, (slot, at) in enumerate(pieces(j)):
            low = (scores[slot, at] * (probs[slot, at] - grad_dot)).astype(bf16)
            ds_low[j * 2 * group + i * piece : j * 2 * group + (i + 1) * piece] = low
        at = slice(j * 2 * group, (j + 1) * 2 * group)
        item = jnp.dot(ds_low[at], q_low[...], preferred_element_type=f32)
        hops[z_count + j] = first_hop(z_count + j, item, j % 2 == 1)

    def query_part(half):
        cols = slice(half * rows, (half + 1) * rows)
        return contract_first(ds_low[:, cols], k_sorted[...])

    later = {}

    def onward(u):
        later[u] = second_hop(u, hops[u])

    last = z_count - 1
    key_part(0)
    key_part(1)
    onward(0)
    key_part(2)
    onward(1)
    onward(2)
    value_part(last)
    key_part(last)
    for j in range(last):
        onward(z_count + j)
        third_hop(j, later[j])
    gq_out[...] = (query_part(1) * scaling).astype(bf16)
    gq_copy = remote(gq_out, gq_in, partner)
    for j in range(last):
        third_hop(z_count + j, later[z_count + j])
    onward(last)
    onward(z_count + last)
    grad_query = query_part(0)
    gq_copy.wait_recv()
    gq_ref[...] = (grad_query * scaling + gq_in[...].astype(f32)).astype(bf16)
    value_sum = third_hop(last, later[last])
    for d in range(last):
        z_copy(0, 0, d).wait_recv()
        value_sum = value_sum + z_in[0, d].astype(f32)
    gv_ref[...] = value_sum
    key_sum = third_hop(z_count + last, later[z_count + last])
    for d in range(last):
        z_copy(1, 0, d).wait_recv()
        key_sum = key_sum + z_in[1, d].astype(f32)
    gk_ref[...] = key_sum
    for copy in issued + z_copies_out:
        copy.wait_send()


def store_kernel(*refs):
    copies = [
        pltpu.make_async_copy(refs[i], refs[3 + i], refs[6].at[i]) for i in range(3)
    ]
    for copy in copies:
        copy.start()
    for copy in copies:
        copy.wait()


def fused_device(queries, keys, values, d_out, doc_lengths, fold_order):
    z_count = lax.axis_size("head") // 2
    _, rows, width = queries.shape
    group = rows // z_count
    piece = group // 2
    units = 2 * z_count
    low, full = jnp.bfloat16, jnp.float32
    vmem = pl.BlockSpec(memory_space=pltpu.VMEM)
    copies = 4 + 2 + 4 + 2 + 2 * units + 1
    hbm = pl.BlockSpec(memory_space=pltpu.HBM)
    grad_query, grad_key, grad_value = pl.pallas_call(
        functools.partial(fused_kernel, z_count),
        out_shape=(
            pltpu.VMEM((rows, width), low),
            pltpu.VMEM((piece, width), full),
            pltpu.VMEM((piece, width), full),
        ),
        in_specs=[hbm] * 6,
        out_specs=(vmem,) * 3,
        scratch_shapes=[
            pltpu.VMEM((2 * rows, width), low),
            pltpu.VMEM((2 * rows, width), low),
            pltpu.VMEM((2 * rows, width), low),
            pltpu.SMEM(doc_lengths.shape, jnp.int32),
            pltpu.SMEM(fold_order.shape, jnp.int32),
            pltpu.SemaphoreType.DMA((6,)),
            pltpu.VMEM((2, 2, rows, width), low),
            pltpu.VMEM((2, rows, 2 * rows), full),
            pltpu.VMEM((2, rows, 2 * rows), full),
            pltpu.VMEM((2, 4, 1, 2 * rows), full),
            pltpu.VMEM((z_count, 2 * group, 2 * rows), low),
            pltpu.VMEM((2 * rows, 2 * rows), low),
            pltpu.VMEM((2 * rows, width), low),
            pltpu.VMEM((2, 1, 2 * rows), full),
            pltpu.VMEM((2, 1, 2 * rows), full),
            pltpu.VMEM((units, group, width), full),
            pltpu.VMEM((units, group, width), low),
            pltpu.VMEM((units, group, width), low),
            pltpu.VMEM((units, piece, width), low),
            pltpu.VMEM((units, piece, width), low),
            pltpu.VMEM((2, z_count - 1, piece, width), low),
            pltpu.VMEM((2, z_count - 1, piece, width), low),
            pltpu.VMEM((rows, width), low),
            pltpu.VMEM((rows, width), low),
            pltpu.SemaphoreType.DMA((copies,)),
            pltpu.SemaphoreType.DMA((copies,)),
            pltpu.SemaphoreType.DMA((2, z_count - 1)),
            pltpu.SemaphoreType.DMA((2, z_count - 1)),
            pltpu.SemaphoreType.REGULAR((z_count - 2,)),
        ],
        compiler_params=pltpu.CompilerParams(
            collective_id=0, has_side_effects=True, vmem_limit_bytes=60 * 1024 * 1024
        ),
        name="fused_grads",
    )(
        *(
            pltpu.with_memory_space_constraint(item, pltpu.HBM)
            for item in (
                queries[0], keys[0], values[0], d_out[0], doc_lengths, fold_order
            )
        )
    )
    outs = (grad_query, grad_key, grad_value)
    outs = pl.pallas_call(
        store_kernel,
        out_shape=tuple(jax.ShapeDtypeStruct(item.shape, item.dtype) for item in outs),
        in_specs=[vmem] * 3,
        out_specs=(hbm,) * 3,
        scratch_shapes=[pltpu.SemaphoreType.DMA((3,))],
        compiler_params=pltpu.CompilerParams(vmem_limit_bytes=4 * 1024 * 1024),
        name="store_grads",
    )(*outs)
    return tuple(item[None] for item in outs)


def solution(mesh):
    in_specs = (
        P("head", "seq", None),
        P(None, "seq", None),
        P(None, "seq", None),
        P("head", "seq", None),
        P(),
        P(),
    )
    out_specs = (
        P("head", "seq", None),
        P(None, ("seq", "head"), None),
        P(None, ("seq", "head"), None),
    )
    small = mesh.shape["seq"] == 4 and mesh.shape["head"] == HEAD_COUNT
    return jax.shard_map(
        fused_device if small else per_device,
        mesh=mesh,
        in_specs=in_specs,
        out_specs=out_specs,
        check_vma=False,
    )
```
